32 devices in a mesh: head: 4 (over z), outer: 2 (over core), inner: 4 (over y, x).
Axes of the slice: x: 2, y: 2, z: 4, core: 2. Of those that a mesh axis runs over, the one named last changes fastest.
Arguments:
- query: bfloat16 [4096, 8192], P(('outer', 'inner', 'head')), may hold values from -100 to 100
- keys: bfloat16 [4096, 1024], P(('outer', 'inner', 'head')), may hold values from -4.5 to 4.5
- values: bfloat16 [4096, 1024], P(('outer', 'inner', 'head')), may hold values from -6 to 6
- lengths: int32 [8], replicated, may hold values from 1 to 1024, 4096 in all
Outputs:
- attended: bfloat16 [4096, 8192], P(('outer', 'inner', 'head'))
The draws below stay inside these ranges and needn't reach their ends.
Inputs may be any that keep to these rules, and one draw needn't show every extreme that they name: `lengths`: they sum to 4096, and the longest is exactly 1024.
All inputs are finite; a program needn't handle non-finite values.
Results may differ from the reference program's by a relative error of at most 0.0038.
Values may be sent and summed in bfloat16 or wider, within the bound.
A program may use at most 64 MiB of HBM per device.

```python
import math
import jax
import jax.numpy as jnp
import numpy as np
from jax import lax

QUERY_HEAD_COUNT = 64
KEY_VALUE_HEADS = 8
HEAD_SIZE = 128
NEARBY_TOKENS = 512
PACKED_TOKENS = 4096
REACH = 2
MAXDOC = 1024
NDOCS = 8


def starting_keys(key):
    sampled = jnp.clip(jax.random.normal(jax.random.fold_in(key, 30), (PACKED_TOKENS, KEY_VALUE_HEADS * HEAD_SIZE), jnp.float32), -4.5, 4.5)
    return sampled


def draw_keys(key, part):
    return starting_keys(key).astype(jnp.bfloat16)


def draw_query(key, part):
    result = jnp.clip(jax.random.normal(jax.random.fold_in(key, 40), (PACKED_TOKENS, QUERY_HEAD_COUNT * HEAD_SIZE), jnp.float32), -4.5, 4.5)
    return result.astype(jnp.bfloat16)


def block_levels(key, shape, shards, low, high):
    factor_of = 1.0
    for axis_at, parts in shards:
        steps = jax.random.uniform(jax.random.fold_in(jax.random.fold_in(key, 6), axis_at), (parts,), jnp.float32, low / len(shards), high / len(shards))
        factor_of = factor_of * jnp.repeat(jnp.exp(steps), shape[axis_at] // parts).reshape((-1,) + (1,) * (len(shape) - 1 - axis_at))
    return factor_of


def split_up(amount, total, limit, skew):
    loads = [(1 << 20) // math.isqrt(rank ** skew) + 1 for rank in range(2, amount + 1)]
    rest, given = total - limit - (amount - 1), [1] * (amount - 1)
    while rest > 0:
        candidates = [i for i in range(amount - 1) if given[i] < limit]
        pool, remaining = sum([loads[i] for i in candidates]), rest
        for i in candidates:
            addition = min(limit - given[i], max(1, remaining * loads[i] // pool), rest)
            given[i] = given[i] + addition
            rest = rest - addition
    return np.array([limit] + given)


def uneven_parts(stream_key, amount, total, most, lean):
    if amount == 2:
        one = jax.random.randint(stream_key, (), max(1, total - most), min(most, total - 1) + 1)
        return jnp.stack([one, total - one])
    sizes = jnp.asarray(split_up(amount, total, most, lean), jnp.int32)
    twos = (amount - 1) // 2
    donor, taker = sizes[1:1 + 2 * twos:2], sizes[2:2 + 2 * twos:2]
    margin = jnp.minimum(donor - 1, most - taker)
    shifted = jax.random.randint(jax.random.fold_in(stream_key, 1), (twos,), 0, 1 << 20) % (margin + 1)
    sizes = sizes.at[1:1 + 2 * twos:2].set(donor - shifted).at[2:2 + 2 * twos:2].set(taker + shifted)
    return sizes[jax.random.permutation(jax.random.fold_in(stream_key, 2), amount)]


def scatter_about(own_key, extent, deviation, reach, pieces=(), kind=jnp.bfloat16):
    level = block_levels(own_key, extent, pieces, -0.22, 0.18) if pieces else 1.0
    drawn = jax.random.normal(own_key, extent, jnp.float32) * deviation * level
    return jnp.minimum(jnp.maximum(drawn, -reach), reach).astype(kind)


def setup_inputs(seed: int = 0) -> dict:
    streams_of = jax.random.split(jax.random.key(seed), 5)
    query = draw_query(jax.random.fold_in(streams_of[4], 71), 0)
    keys = draw_keys(jax.random.fold_in(streams_of[4], 71), 0)
    values = scatter_about(streams_of[2], (PACKED_TOKENS, KEY_VALUE_HEADS * HEAD_SIZE), 1.0, 6.0, ((0, 32),))
    lengths = uneven_parts(streams_of[3], NDOCS, PACKED_TOKENS, MAXDOC, 2).astype(jnp.int32)
    return dict(query=query, keys=keys, values=values, lengths=lengths)


def doc_of(lengths, positions):
    ends = jnp.cumsum(lengths)
    return lax.optimization_barrier(jnp.sum((positions[:, None] >= ends[None, :]).astype(jnp.int32), axis=1))

def reference(query, keys, values, lengths):
    group_width = QUERY_HEAD_COUNT // KEY_VALUE_HEADS
    trailing_length = REACH * NEARBY_TOKENS
    key_length = trailing_length + NEARBY_TOKENS
    score_scale = 1.0 / math.sqrt(HEAD_SIZE)
    positions = lax.iota(jnp.int32, PACKED_TOKENS)
    docs = doc_of(lengths, positions)
    filled_keys = jnp.concatenate([jnp.zeros((trailing_length, KEY_VALUE_HEADS * HEAD_SIZE), jnp.bfloat16), keys], 0)
    filled_values = jnp.concatenate([jnp.zeros((trailing_length, KEY_VALUE_HEADS * HEAD_SIZE), jnp.bfloat16), values], 0)
    padded_docs = jnp.concatenate([jnp.full((trailing_length,), -1, jnp.int32), docs], 0)

    def one_block(block_index):
        start_row = (block_index * NEARBY_TOKENS).astype(jnp.int32)
        query_matrix = lax.dynamic_slice_in_dim(query, start_row, NEARBY_TOKENS, 0).astype(jnp.float32)
        query_matrix = query_matrix.reshape(NEARBY_TOKENS, KEY_VALUE_HEADS, group_width, HEAD_SIZE)
        key_matrix = lax.dynamic_slice_in_dim(filled_keys, start_row, key_length, 0).astype(jnp.float32)
        key_matrix = key_matrix.reshape(key_length, KEY_VALUE_HEADS, HEAD_SIZE)
        value_matrix = lax.dynamic_slice_in_dim(filled_values, start_row, key_length, 0).astype(jnp.float32)
        value_matrix = value_matrix.reshape(key_length, KEY_VALUE_HEADS, HEAD_SIZE)
        query_docs = lax.dynamic_slice_in_dim(docs, start_row, NEARBY_TOKENS, 0)
        key_docs = lax.dynamic_slice_in_dim(padded_docs, start_row, key_length, 0)
        query_pos = start_row + lax.iota(jnp.int32, NEARBY_TOKENS)
        key_pos = start_row - trailing_length + lax.iota(jnp.int32, key_length)
        visible = (query_docs[:, None] == key_docs[None, :]) & (key_pos[None, :] <= query_pos[:, None])

        def one_head(operands):
            query_heads, key_heads, value_heads = operands
            scores = jnp.einsum('qgd,cd->gqc', query_heads, key_heads) * score_scale
            masked = jnp.where(visible[None], scores, -1e+30)
            top = lax.optimization_barrier(jnp.max(masked, axis=2))
            weights = jnp.where(visible[None], jnp.exp(masked - top[..., None]), 0.0)
            total = lax.optimization_barrier(jnp.sum(weights, axis=2))
            rounded = lax.optimization_barrier(weights.astype(jnp.bfloat16)).astype(jnp.float32)
            summed = jnp.einsum('gqc,cd->qgd', rounded, value_heads)
            return summed / jnp.transpose(total, (1, 0))[..., None]
        per_head = lax.map(one_head, (jnp.transpose(query_matrix, (1, 0, 2, 3)), jnp.transpose(key_matrix, (1, 0, 2)), jnp.transpose(value_matrix, (1, 0, 2))))
        return jnp.transpose(per_head, (1, 0, 2, 3)).reshape(NEARBY_TOKENS, QUERY_HEAD_COUNT * HEAD_SIZE).astype(jnp.bfloat16)
    blocks = lax.map(one_block, lax.iota(jnp.int32, PACKED_TOKENS // NEARBY_TOKENS))
    return blocks.reshape(PACKED_TOKENS, QUERY_HEAD_COUNT * HEAD_SIZE)
```

```python
import functools
import math

import jax
import jax.numpy as jnp
from jax import lax
from jax.experimental import pallas as pl
from jax.experimental.pallas import tpu as pltpu
from jax.sharding import PartitionSpec as P

HEAD_SIZE = 128
MESH = pl.DeviceIdType.MESH
BOTH, KEY, VALUE = pl.ds(0, 2), pl.ds(0, 1), pl.ds(1, 1)

TIMES = {
    "x own": (-30.16, -10.38),
    "y own": (-93.89, 0.80),
    "z mate": (-51.39, 15.57),
    "z own": (-16.10, 15.74),
    "z1": (16.36, 9.42),
    "z2": (24.86, 12.85),
    "z3": (44.16, 11.37),
    "y0": (13.69, 1.81),
    "y1": (31.15, 9.42),
    "y2": (45.44, 12.20),
    "y3": (54.66, 11.66),
    "x0": (45.67, 11.75),
    "compute": (66.38, 11.77),
}


def order_of(heads, groups, period):
    steps = []
    for name, (first, later) in TIMES.items():
        for g in range(groups):
            at = first + later * g
            if name == "compute":
                steps += [(at + later * j / period, 0, name, g, j) for j in range(period)]
                continue

            steps.append((at, 1, name, g, 0))
            if name in ("z3", "y3"):
                steps += [(at, d, name[0] + str(d), g, 0) for d in range(4, heads)]

    slots = [[]]
    for _, _, name, g, j in sorted(steps, key=lambda step: step[:2]):
        if name != "compute":
            slots[-1].append((name, g))
            continue

        if j == 0:
            slots[-1].append(("ready", g))
        slots.append([])
    return slots


def kernel(
    heads, outers, inners, lengths_ref, q_hbm, k_ref, v_ref, out_hbm,
    q_ref, out_ref, kv, bias, q_sem, out_sem, own_sem,
    z_send, z_recv, on_send, y_send, y_recv, x_send, x_recv, pair_send, pair_recv,
):
    tokens = q_ref.shape[0]
    groups = k_ref.shape[1] // HEAD_SIZE
    width = q_ref.shape[1] // k_ref.shape[1]
    pair = 2 if width % 2 == 0 else 1
    period = width // pair
    block = heads * tokens
    contexts = outers * inners
    span = (2 * heads + 1) * tokens
    me = lax.axis_index("head")
    ctx = lax.axis_index("outer") * inners + lax.axis_index("inner")
    odd = lax.rem(ctx, 2)
    side = lax.rem(me, 2)
    mate = me + 1 - 2 * side

    def context(steps):
        at = lax.rem(ctx + steps + contexts, contexts)
        return {"outer": at // inners, "inner": lax.rem(at, inners)}

    partner = context(1 - 2 * odd)

    def shard_of(k):
        other = lax.rem(me // 2 + k // 2, heads // 2)
        return 2 * other + (side if k % 2 == 0 else 1 - side)

    shards = [shard_of(k) for k in range(heads)]
    distances = [jnp.abs(shard - me) for shard in shards]

    def rows(at, shard):
        return pl.ds(pl.multiple_of(at * block + shard * tokens, tokens), tokens)

    def part_of(k):
        return KEY if k == 1 else BOTH

    def own_copy(g, which):
        ref = (k_ref, v_ref)[which]
        return pltpu.make_async_copy(
            ref.at[:, pl.ds(pl.multiple_of(g * HEAD_SIZE, HEAD_SIZE), HEAD_SIZE)],
            kv.at[g, which, rows(2, me), :],
            own_sem.at[which, g],
        )

    def remote(g, part, source, landing, send, recv, place):
        return pltpu.make_async_remote_copy(
            src_ref=kv.at[g, part, source, :], dst_ref=kv.at[g, part, landing, :],
            send_sem=send, recv_sem=recv, device_id=place, device_id_type=MESH,
        )

    def z_own(g, k, part):
        at = rows(2, me)
        slot = (1 if k == 1 and part is VALUE else 0, k, g)
        recv = (1 if k == 1 and part is VALUE else 0, me, g)
        return remote(g, part, at, at, z_send.at[slot], z_recv.at[recv], {"head": shards[k]})

    def z_on(g, k):
        at = rows(2, shards[k])
        to = jnp.clip(me + jnp.where(shards[k] < me, 1, -1), 0, heads - 1)
        return remote(
            g, BOTH, at, at, on_send.at[k, g], z_recv.at[0, shards[k], g], {"head": to}
        )

    def z_goes_on(k):
        beyond = jnp.where(shards[k] < me, me + 1 < heads, me >= 1)
        return (distances[k] >= 2) & beyond

    def z_arrival(g, k, part):
        at = rows(2, shards[k])
        recv = (1 if k == 1 and part is VALUE else 0, shards[k], g)
        return remote(g, part, at, at, on_send.at[k, g], z_recv.at[recv], {"head": mate})

    def y_copy(g, k):
        return remote(
            g, part_of(k), rows(2, shards[k]), rows(0, shards[k]),
            y_send.at[k, g], y_recv.at[k, g], context(2),
        )

    def x_copy(g, k):
        return remote(
            g, part_of(k), rows(2 * (1 - odd), shards[k]), rows(1, shards[k]),
            x_send.at[k, g], x_recv.at[k, g], partner,
        )

    def pair_copy(g, at):
        return remote(
            g, VALUE, rows(at, me), rows(at, me), pair_send.at[at, g], pair_recv.at[at, g],
            {"head": mate},
        )

    def pair_arrival(g, at):
        return remote(
            g, VALUE, rows(at, mate), rows(at, mate), pair_send.at[at, g], pair_recv.at[at, g],
            {"head": mate},
        )

    def y_needed(k):
        return (odd == 1) | (shards[k] >= me)

    def have(g, k):
        @pl.when(y_needed(k))
        def _():
            y_copy(g, k).start()

        @pl.when(odd == 0)
        def _():
            x_copy(g, k).start()

    def x_own_event(g):
        @pl.when(odd == 0)
        def _():
            x_copy(g, 0).start()

    def y_own_event(g):
        y_copy(g, 0).start()

    def mate_event(g):
        @pl.when(side == 0)
        def _():
            z_own(g, 1, VALUE).start()

        z_own(g, 1, KEY).start()

    def z_own_event(g):
        for k in range(2, heads):
            @pl.when(distances[k] <= 2)
            def _():
                z_own(g, k, BOTH).start()

    def z_mate_event(g):
        z_arrival(g, 1, KEY).wait_recv()

        @pl.when(side == 1)
        def _():
            z_arrival(g, 1, VALUE).wait_recv()

        have(g, 1)

    def z_event(g, distance):
        for k in range(2, heads):
            @pl.when(jnp.maximum(distances[k], 2) == distance)
            def _():
                z_arrival(g, k, BOTH).wait_recv()

                @pl.when(z_goes_on(k))
                def _():
                    z_on(g, k).start()

                have(g, k)

    def y_step(g, k):
        @pl.when(y_needed(k))
        def _():
            y_copy(g, k).wait_recv()

        @pl.when(odd == 1)
        def _():
            x_copy(g, k).start()

        if k == 0:
            @pl.when(side == 1)
            def _():
                pair_copy(g, 0).start()

    def y_event(g, distance):
        for k in range(2, heads):
            @pl.when(jnp.maximum(distances[k], 2) == distance)
            def _():
                y_step(g, k)

    def x_event(g):
        x_copy(g, 0).wait_recv()
        pair_copy(g, 1).start()

    def final_event(g):
        for k in range(1, heads):
            x_copy(g, k).wait_recv()
        pair_arrival(g, 1).wait_recv()

        @pl.when(side == 0)
        def _():
            pair_arrival(g, 0).wait_recv()

    actions = {
        "x own": x_own_event, "y own": y_own_event, "z mate": mate_event, "z own": z_own_event,
        "z1": z_mate_event, "y0": functools.partial(y_step, k=0),
        "y1": functools.partial(y_step, k=1), "x0": x_event, "ready": final_event,
    }
    for distance in range(2, heads):
        actions["z" + str(distance)] = functools.partial(z_event, distance=distance)
        actions["y" + str(distance)] = functools.partial(y_event, distance=distance)

    slots = order_of(heads, groups, period)
    loads = list(dict.fromkeys(g for slot in slots for name, g in slot if "own" in name or "mate" in name))

    q_copy = pltpu.make_async_copy(q_hbm, q_ref, q_sem)
    for g in loads:
        own_copy(g, 0).start()
        own_copy(g, 1).start()
    q_copy.start()

    barrier = pltpu.get_barrier_semaphore()
    for distance in range(1, heads):
        pl.semaphore_signal(
            barrier, inc=1, device_id={"head": lax.rem(me + distance, heads)}, device_id_type=MESH
        )
    for place in (context(2), context(-2), partner):
        pl.semaphore_signal(barrier, inc=1, device_id=place, device_id_type=MESH)
    pl.semaphore_wait(barrier, heads - 1 + 3)

    def fill_bias():
        first = ctx * block + me * tokens
        query_pos = first + lax.broadcasted_iota(jnp.int32, (tokens, span), 0)
        key_pos = first - 2 * block + lax.broadcasted_iota(jnp.int32, (tokens, span), 1)
        row_pos = first + lax.broadcasted_iota(jnp.int32, (tokens, 128), 0)
        begin = jnp.zeros((tokens, 128), jnp.int32)
        end = jnp.int32(0)
        for n in range(lengths_ref.shape[0]):
            end = end + lengths_ref[n]
            begin = jnp.where(row_pos >= end, end, begin)
        visible = (key_pos >= begin[:, :1]) & (key_pos <= query_pos)
        bias[...] = jnp.where(visible, 0.0, -1e30)

    factor = math.log2(math.e) / math.sqrt(HEAD_SIZE)
    reading = pl.ds(pl.multiple_of(me * tokens, tokens), span)

    def out_copy(g):
        at = pl.ds(pl.multiple_of(g * width * HEAD_SIZE, HEAD_SIZE), width * HEAD_SIZE)
        return pltpu.make_async_copy(out_ref.at[:, at], out_hbm.at[:, at], out_sem.at[g])

    def compute(g, j):
        key_part = kv.at[g, 0]
        value_part = kv.at[g, 1]
        at = (g * width + j * pair) * HEAD_SIZE
        columns = [
            pl.ds(pl.multiple_of(at + p * HEAD_SIZE, HEAD_SIZE), HEAD_SIZE) for p in range(pair)
        ]
        q = jnp.concatenate([q_ref[:, c] for c in columns], axis=0)
        scores = lax.dot_general(
            q, key_part[reading, :], (((1,), (1,)), ((), ())), preferred_element_type=jnp.float32
        )
        scores = scores.reshape(pair, tokens, span) + bias[...][None]
        scores = scores.reshape(pair * tokens, span)
        top = jnp.max(scores, axis=1, keepdims=True)
        weights = jnp.exp2((scores - top) * factor)
        total = jnp.sum(weights, axis=1, keepdims=True)
        summed = jnp.dot(
            weights.astype(jnp.bfloat16), value_part[reading, :],
            preferred_element_type=jnp.float32,
        )
        result = (summed / total).astype(out_ref.dtype)
        for p in range(pair):
            out_ref[:, columns[p]] = result[p * tokens:(p + 1) * tokens]

    loaded = set()

    def take(slot):
        for name, g in slot:
            if g not in loaded:
                loaded.add(g)
                own_copy(g, 0).wait()
                own_copy(g, 1).wait()
            actions[name](g)

    def dispatch(step, low, high):
        if not any(slots[low:high]):
            return

        if high - low == 1:
            take(slots[low])
            return

        middle = (low + high) // 2

        @pl.when(step < middle)
        def _():
            dispatch(step, low, middle)

        @pl.when(step >= middle)
        def _():
            dispatch(step, middle, high)

    take(slots[0][:groups])
    fill_bias()
    take(slots[0][groups:])
    q_copy.wait()

    def group_step(g, carry):
        def head_step(j, carry):
            compute(g, j)
            dispatch(g * period + j + 1, 1, groups * period + 1)
            return carry

        lax.fori_loop(0, period, head_step, 0)
        out_copy(g).start()
        return carry

    lax.fori_loop(0, groups, group_step, 0)

    def drain(g, carry):
        z_own(g, 1, KEY).wait_send()

        @pl.when(side == 0)
        def _():
            z_own(g, 1, VALUE).wait_send()

        for k in range(2, heads):
            @pl.when(distances[k] <= 2)
            def _():
                z_own(g, k, BOTH).wait_send()

            @pl.when(z_goes_on(k))
            def _():
                z_on(g, k).wait_send()

        for k in range(heads):
            @pl.when(y_needed(k))
            def _():
                y_copy(g, k).wait_send()

            x_copy(g, k).wait_send()

        pair_copy(g, 1).wait_send()

        @pl.when(side == 1)
        def _():
            pair_copy(g, 0).wait_send()

        out_copy(g).wait()
        return carry

    lax.fori_loop(0, groups, drain, 0)


def solution(mesh):
    heads, outers, inners = (mesh.shape[name] for name in ("head", "outer", "inner"))

    def per_device(query, keys, values, lengths):
        tokens = query.shape[0]
        groups = keys.shape[1] // HEAD_SIZE
        sems = pltpu.SemaphoreType.DMA
        return pl.pallas_call(
            functools.partial(kernel, heads, outers, inners),
            out_shape=jax.ShapeDtypeStruct(query.shape, query.dtype),
            in_specs=[
                pl.BlockSpec(memory_space=pltpu.SMEM),
                pl.BlockSpec(memory_space=pl.ANY),
                pl.BlockSpec(memory_space=pl.ANY),
                pl.BlockSpec(memory_space=pl.ANY),
            ],
            out_specs=pl.BlockSpec(memory_space=pl.ANY),
            scratch_shapes=[
                pltpu.VMEM(query.shape, query.dtype),
                pltpu.VMEM(query.shape, query.dtype),
                pltpu.VMEM((groups, 2, 3 * heads * tokens, HEAD_SIZE), jnp.bfloat16),
                pltpu.VMEM((tokens, (2 * heads + 1) * tokens), jnp.float32),
                sems,
                sems((groups,)),
                sems((2, groups)),
                sems((2, heads, groups)),
                sems((2, heads, groups)),
                sems((heads, groups)),
                sems((heads, groups)),
                sems((heads, groups)),
                sems((heads, groups)),
                sems((heads, groups)),
                sems((2, groups)),
                sems((2, groups)),
            ],
            compiler_params=pltpu.CompilerParams(collective_id=0, has_side_effects=True),
        )(lengths, query, keys, values)

    rows = P(("outer", "inner", "head"), None)
    return jax.shard_map(
        per_device,
        mesh=mesh,
        in_specs=(rows, rows, rows, P()),
        out_specs=rows,
        check_vma=False,
    )
```

```python
import functools
import math

import jax
import jax.numpy as jnp
from jax import lax
from jax.experimental import pallas as pl
from jax.experimental.pallas import tpu as pltpu
from jax.sharding import PartitionSpec as P

HEAD_SIZE = 128
MESH = pl.DeviceIdType.MESH
BOTH, KEY, VALUE = pl.ds(0, 2), pl.ds(0, 1), pl.ds(1, 1)

TIMES = {
    "x own": (-0.79, -14.57),
    "y own": (-250.76, 11.43),
    "z mate": (-54.63, 3.55),
    "z own": (-56.68, 24.08),
    "z1": (-23.74, 8.00),
    "z2": (13.60, 18.83),
    "z3": (33.48, 17.76),
    "y0": (-28.36, 8.15),
    "y1": (15.77, 5.69),
    "y2": (47.00, 17.93),
    "y3": (57.14, 17.66),
    "x0": (38.87, 20.69),
    "compute": (77.81, 17.72),
}


def order_of(heads, groups, period):
    steps = []
    for name, (first, later) in TIMES.items():
        for g in range(groups):
            at = first + later * g
            if name == "compute":
                steps += [(at + later * j / period, 0, name, g, j) for j in range(period)]
                continue

            steps.append((at, 1, name, g, 0))
            if name in ("z3", "y3"):
                steps += [(at, d, name[0] + str(d), g, 0) for d in range(4, heads)]

    slots = [[]]
    for _, _, name, g, j in sorted(steps, key=lambda step: step[:2]):
        if name != "compute":
            slots[-1].append((name, g))
            continue

        if j == 0:
            slots[-1].append(("ready", g))
        slots.append([])
    return slots


def pair_of(width):
    return 2 if width % 8 == 0 else 1


def kernel(
    heads, outers, inners, lengths_ref, q_hbm, k_ref, v_ref, out_ref,
    q_ref, kv, bias, held, tops, totals, rounded, q_sem, own_sem,
    z_send, z_recv, on_send, y_send, y_recv, x_send, x_recv, pair_send, pair_recv,
):
    tokens = q_ref.shape[0]
    groups = k_ref.shape[1] // HEAD_SIZE
    width = q_ref.shape[1] // k_ref.shape[1]
    pair = pair_of(width)
    period = width // pair
    steps = groups * period
    block = heads * tokens
    contexts = outers * inners
    span = (2 * heads + 1) * tokens
    me = lax.axis_index("head")
    ctx = lax.axis_index("outer") * inners + lax.axis_index("inner")
    odd = lax.rem(ctx, 2)
    side = lax.rem(me, 2)
    mate = me + 1 - 2 * side

    def context(steps):
        at = lax.rem(ctx + steps + contexts, contexts)
        return {"outer": at // inners, "inner": lax.rem(at, inners)}

    partner = context(1 - 2 * odd)

    def shard_of(k):
        other = lax.rem(me // 2 + k // 2, heads // 2)
        return 2 * other + (side if k % 2 == 0 else 1 - side)

    shards = [shard_of(k) for k in range(heads)]
    distances = [jnp.abs(shard - me) for shard in shards]

    def rows(at, shard):
        return pl.ds(pl.multiple_of(at * block + shard * tokens, tokens), tokens)

    def part_of(k):
        return KEY if k == 1 else BOTH

    def own_copy(g, which):
        ref = (k_ref, v_ref)[which]
        return pltpu.make_async_copy(
            ref.at[:, pl.ds(pl.multiple_of(g * HEAD_SIZE, HEAD_SIZE), HEAD_SIZE)],
            kv.at[g, which, rows(2, me), :],
            own_sem.at[which, g],
        )

    def remote(g, part, source, landing, send, recv, place):
        return pltpu.make_async_remote_copy(
            src_ref=kv.at[g, part, source, :], dst_ref=kv.at[g, part, landing, :],
            send_sem=send, recv_sem=recv, device_id=place, device_id_type=MESH,
        )

    def z_own(g, k, part):
        at = rows(2, me)
        slot = (1 if k == 1 and part is VALUE else 0, k, g)
        recv = (1 if k == 1 and part is VALUE else 0, me, g)
        return remote(g, part, at, at, z_send.at[slot], z_recv.at[recv], {"head": shards[k]})

    def z_on(g, k):
        at = rows(2, shards[k])
        to = jnp.clip(me + jnp.where(shards[k] < me, 1, -1), 0, heads - 1)
        return remote(
            g, BOTH, at, at, on_send.at[k, g], z_recv.at[0, shards[k], g], {"head": to}
        )

    def z_goes_on(k):
        beyond = jnp.where(shards[k] < me, me + 1 < heads, me >= 1)
        return (distances[k] >= 2) & beyond

    def z_arrival(g, k, part):
        at = rows(2, shards[k])
        recv = (1 if k == 1 and part is VALUE else 0, shards[k], g)
        return remote(g, part, at, at, on_send.at[k, g], z_recv.at[recv], {"head": mate})

    def y_copy(g, k):
        return remote(
            g, part_of(k), rows(2, shards[k]), rows(0, shards[k]),
            y_send.at[k, g], y_recv.at[k, g], context(2),
        )

    def x_copy(g, k):
        return remote(
            g, part_of(k), rows(2 * (1 - odd), shards[k]), rows(1, shards[k]),
            x_send.at[k, g], x_recv.at[k, g], partner,
        )

    def pair_copy(g, at):
        return remote(
            g, VALUE, rows(at, me), rows(at, me), pair_send.at[at, g], pair_recv.at[at, g],
            {"head": mate},
        )

    def pair_arrival(g, at):
        return remote(
            g, VALUE, rows(at, mate), rows(at, mate), pair_send.at[at, g], pair_recv.at[at, g],
            {"head": mate},
        )

    def y_needed(k):
        return (odd == 1) | (shards[k] >= me)

    def have(g, k):
        @pl.when(y_needed(k))
        def _():
            y_copy(g, k).start()

        @pl.when(odd == 0)
        def _():
            x_copy(g, k).start()

    def x_own_event(g):
        @pl.when(odd == 0)
        def _():
            x_copy(g, 0).start()

    def y_own_event(g):
        y_copy(g, 0).start()

    def mate_event(g):
        @pl.when(side == 0)
        def _():
            z_own(g, 1, VALUE).start()

        z_own(g, 1, KEY).start()

    def z_own_event(g):
        for k in range(2, heads):
            @pl.when(distances[k] <= 2)
            def _():
                z_own(g, k, BOTH).start()

    def z_mate_event(g):
        z_arrival(g, 1, KEY).wait_recv()

        @pl.when(side == 1)
        def _():
            z_arrival(g, 1, VALUE).wait_recv()

        have(g, 1)

    def z_event(g, distance):
        for k in range(2, heads):
            @pl.when(jnp.maximum(distances[k], 2) == distance)
            def _():
                z_arrival(g, k, BOTH).wait_recv()

                @pl.when(z_goes_on(k))
                def _():
                    z_on(g, k).start()

                have(g, k)

    def y_step(g, k):
        @pl.when(y_needed(k))
        def _():
            y_copy(g, k).wait_recv()

        @pl.when(odd == 1)
        def _():
            x_copy(g, k).start()

        if k == 0:
            @pl.when(side == 1)
            def _():
                pair_copy(g, 0).start()

    def y_event(g, distance):
        for k in range(2, heads):
            @pl.when(jnp.maximum(distances[k], 2) == distance)
            def _():
                y_step(g, k)

    def x_event(g):
        x_copy(g, 0).wait_recv()
        pair_copy(g, 1).start()

    def final_event(g):
        for k in range(1, heads):
            x_copy(g, k).wait_recv()
        pair_arrival(g, 1).wait_recv()

        @pl.when(side == 0)
        def _():
            pair_arrival(g, 0).wait_recv()

    actions = {
        "x own": x_own_event, "y own": y_own_event, "z mate": mate_event, "z own": z_own_event,
        "z1": z_mate_event, "y0": functools.partial(y_step, k=0),
        "y1": functools.partial(y_step, k=1), "x0": x_event, "ready": final_event,
    }
    for distance in range(2, heads):
        actions["z" + str(distance)] = functools.partial(z_event, distance=distance)
        actions["y" + str(distance)] = functools.partial(y_event, distance=distance)

    slots = order_of(heads, groups, period)
    loads = list(dict.fromkeys(g for slot in slots for name, g in slot if "own" in name or "mate" in name))

    q_copy = pltpu.make_async_copy(q_hbm, q_ref, q_sem)
    for g in loads:
        own_copy(g, 0).start()
        own_copy(g, 1).start()
    q_copy.start()

    barrier = pltpu.get_barrier_semaphore()
    for distance in range(1, heads):
        pl.semaphore_signal(
            barrier, inc=1, device_id={"head": lax.rem(me + distance, heads)}, device_id_type=MESH
        )
    for place in (context(2), context(-2), partner):
        pl.semaphore_signal(barrier, inc=1, device_id=place, device_id_type=MESH)
    pl.semaphore_wait(barrier, heads - 1 + 3)

    def fill_bias():
        first = ctx * block + me * tokens
        query_pos = first + lax.broadcasted_iota(jnp.int32, (tokens, span), 0)
        key_pos = first - 2 * block + lax.broadcasted_iota(jnp.int32, (tokens, span), 1)
        row_pos = first + lax.broadcasted_iota(jnp.int32, (tokens, 128), 0)
        begin = jnp.zeros((tokens, 128), jnp.int32)
        end = jnp.int32(0)
        for n in range(lengths_ref.shape[0]):
            end = end + lengths_ref[n]
            begin = jnp.where(row_pos >= end, end, begin)
        visible = (key_pos >= begin[:, :1]) & (key_pos <= query_pos)
        bias[...] = jnp.where(visible, 0.0, -1e30)

    factor = math.log2(math.e) / math.sqrt(HEAD_SIZE)
    reading = pl.ds(pl.multiple_of(me * tokens, tokens), span)

    def columns_of(n):
        at = n * pair * HEAD_SIZE
        return [
            pl.ds(pl.multiple_of(at + p * HEAD_SIZE, HEAD_SIZE), HEAD_SIZE) for p in range(pair)
        ]

    def score(n, g, slot):
        q = jnp.concatenate([q_ref[:, c] for c in columns_of(n)], axis=0)
        scores = lax.dot_general(
            q, kv.at[g, 0][reading, :], (((1,), (1,)), ((), ())),
            preferred_element_type=jnp.float32,
        )
        scores = scores.reshape(pair, tokens, span) + bias[...][None]
        scores = scores.reshape(pair * tokens, span)
        held[slot][...] = scores
        tops[slot][...] = jnp.max(scores, axis=1, keepdims=True)

    def weigh(slot):
        weights = jnp.exp2((held[slot][...] - tops[slot][...]) * factor)
        totals[slot][...] = jnp.sum(weights, axis=1, keepdims=True)
        rounded[slot][...] = weights.astype(jnp.bfloat16)

    def attend(n, g, slot):
        summed = jnp.dot(
            rounded[slot][...], kv.at[g, 1][reading, :], preferred_element_type=jnp.float32
        )
        result = (summed / totals[slot][...]).astype(out_ref.dtype)
        for p, c in enumerate(columns_of(n)):
            out_ref[:, c] = result[p * tokens:(p + 1) * tokens]

    loaded = set()

    def take(slot):
        for name, g in slot:
            if g not in loaded:
                loaded.add(g)
                own_copy(g, 0).wait()
                own_copy(g, 1).wait()
            actions[name](g)

    def dispatch(step, low, high):
        if not any(slots[low:high]):
            return

        if high - low == 1:
            take(slots[low])
            return

        middle = (low + high) // 2

        @pl.when(step < middle)
        def _():
            dispatch(step, low, middle)

        @pl.when(step >= middle)
        def _():
            dispatch(step, middle, high)

    take(slots[0][:groups])
    fill_bias()
    take(slots[0][groups:])
    q_copy.wait()

    held[1][...] = jnp.zeros_like(held[1])
    tops[1][...] = jnp.zeros_like(tops[1])
    for slot in range(2):
        totals[slot][...] = jnp.ones_like(totals[slot])
        rounded[slot][...] = jnp.zeros_like(rounded[slot])

    def group_step(g, carry):
        def two_steps(i, carry):
            for slot in range(2):
                n = g * period + 2 * i + slot
                attend(jnp.maximum(n - 2, 0), jnp.maximum(jnp.where(i > 0, g, g - 1), 0), slot)
                weigh(1 - slot)
                score(n, g, slot)
                dispatch(n + 1, 1, steps + 1)
            return carry

        lax.fori_loop(0, period // 2, two_steps, 0)
        return carry

    lax.fori_loop(0, groups, group_step, 0)
    attend(steps - 2, groups - 1, 0)
    weigh(1)
    attend(steps - 1, groups - 1, 1)

    def drain(g, carry):
        z_own(g, 1, KEY).wait_send()

        @pl.when(side == 0)
        def _():
            z_own(g, 1, VALUE).wait_send()

        for k in range(2, heads):
            @pl.when(distances[k] <= 2)
            def _():
                z_own(g, k, BOTH).wait_send()

            @pl.when(z_goes_on(k))
            def _():
                z_on(g, k).wait_send()

        for k in range(heads):
            @pl.when(y_needed(k))
            def _():
                y_copy(g, k).wait_send()

            x_copy(g, k).wait_send()

        pair_copy(g, 1).wait_send()

        @pl.when(side == 1)
        def _():
            pair_copy(g, 0).wait_send()

        return carry

    lax.fori_loop(0, groups, drain, 0)


def solution(mesh):
    heads, outers, inners = (mesh.shape[name] for name in ("head", "outer", "inner"))

    def per_device(query, keys, values, lengths):
        tokens = query.shape[0]
        groups = keys.shape[1] // HEAD_SIZE
        sems = pltpu.SemaphoreType.DMA
        rows = pair_of(query.shape[1] // keys.shape[1]) * tokens
        return pl.pallas_call(
            functools.partial(kernel, heads, outers, inners),
            out_shape=pltpu.VMEM(query.shape, query.dtype),
            in_specs=[
                pl.BlockSpec(memory_space=pltpu.SMEM),
                pl.BlockSpec(memory_space=pl.ANY),
                pl.BlockSpec(memory_space=pl.ANY),
                pl.BlockSpec(memory_space=pl.ANY),
            ],
            out_specs=pl.BlockSpec(memory_space=pltpu.VMEM),
            scratch_shapes=[
                pltpu.VMEM(query.shape, query.dtype),
                pltpu.VMEM((groups, 2, 3 * heads * tokens, HEAD_SIZE), jnp.bfloat16),
                pltpu.VMEM((tokens, (2 * heads + 1) * tokens), jnp.float32),
                [pltpu.VMEM((rows, (2 * heads + 1) * tokens), jnp.float32)] * 2,
                [pltpu.VMEM((rows, 1), jnp.float32)] * 2,
                [pltpu.VMEM((rows, 1), jnp.float32)] * 2,
                [pltpu.VMEM((rows, (2 * heads + 1) * tokens), jnp.bfloat16)] * 2,
                sems,
                sems((2, groups)),
                sems((2, heads, groups)),
                sems((2, heads, groups)),
                sems((heads, groups)),
                sems((heads, groups)),
                sems((heads, groups)),
                sems((heads, groups)),
                sems((heads, groups)),
                sems((2, groups)),
                sems((2, groups)),
            ],
            compiler_params=pltpu.CompilerParams(collective_id=0, has_side_effects=True),
        )(lengths, query, keys, values)

    rows = P(("outer", "inner", "head"), None)
    return jax.shard_map(
        per_device,
        mesh=mesh,
        in_specs=(rows, rows, rows, P()),
        out_specs=rows,
        check_vma=False,
    )
```

```python
import functools
import math

import jax
import jax.numpy as jnp
from jax import lax
from jax.experimental import pallas as pl
from jax.experimental.pallas import tpu as pltpu
from jax.sharding import PartitionSpec as P

HEAD_SIZE = 128
MESH = pl.DeviceIdType.MESH
BOTH, KEY, VALUE = pl.ds(0, 2), pl.ds(0, 1), pl.ds(1, 1)

TIMES = {
    "x own": (-719.83, -349.03),
    "y own": (-829.62, -84.81),
    "z mate": (-730.34, 100.70),
    "z own": (-775.75, 227.04),
    "z1": (-281.24, 103.06),
    "z2": (-53.00, 166.50),
    "z3": (281.86, 145.34),
    "y0": (-88.19, -49.55),
    "y1": (-19.53, 92.10),
    "y2": (348.49, 147.21),
    "y3": (441.94, 155.24),
    "x0": (306.38, 162.83),
    "compute": (656.39, 147.59),
    "z values": (-730.34, 100.70),
    "pair": (-88.19, -49.55),
    "z own odd": (-775.75, 227.04),
    "z2 odd": (-53.00, 166.50),
    "y2 odd": (348.49, 147.21),
}


OWN = ("x own", "y own", "z mate", "z values", "z own", "z own odd")


def order_of(heads, groups, period):
    steps = []
    for name, (first, later) in TIMES.items():
        for g in range(groups):
            at = first + later * g
            at = min(at, TIMES["compute"][0] + TIMES["compute"][1] * g - (name != "compute"))
            if name == "compute":
                steps += [(at + later * j / period, 0, name, g, j) for j in range(period)]
                continue

            if name == "pair":
                at = max(at, TIMES["y0"][0] + TIMES["y0"][1] * g)
            steps.append((at, 2 if name == "pair" else 1, name, g, 0))
            if name in ("z3", "y3"):
                steps += [(at, d, name[0] + str(d), g, 0) for d in range(4, heads)]

    slots = [[]]
    for _, _, name, g, j in sorted(steps, key=lambda step: step[:2]):
        if name != "compute":
            slots[-1].append((name, g))
            continue

        if j == 0:
            slots[-1].append(("ready", g))
        if j == 1 and g > 1:
            slots[-1].append(("drain", g - 2))
        slots.append([])
    return slots


def pair_of(width):
    return 2 if width % 8 == 0 else 1


def kernel(
    heads, outers, inners, lengths_ref, q_hbm, k_ref, v_ref, out_ref,
    q_ref, kv, bias, own_doc, other_doc, held, tops, totals, rounded, q_sem, own_sem,
    z_send, z_recv, on_send, y_send, y_recv, x_send, x_recv, pair_send, pair_recv,
):
    tokens = q_ref.shape[0]
    groups = k_ref.shape[1] // HEAD_SIZE
    width = q_ref.shape[1] // k_ref.shape[1]
    pair = pair_of(width)
    period = width // pair
    steps = groups * period
    block = heads * tokens
    contexts = outers * inners
    span = (2 * heads + 1) * tokens
    me = lax.axis_index("head")
    ctx = lax.axis_index("outer") * inners + lax.axis_index("inner")
    odd = lax.rem(ctx, 2)
    side = lax.rem(me, 2)
    mate = me + 1 - 2 * side

    def context(steps):
        at = lax.rem(ctx + steps + contexts, contexts)
        return {"outer": at // inners, "inner": lax.rem(at, inners)}

    partner = context(1 - 2 * odd)

    def shard_of(k):
        other = lax.rem(me // 2 + k // 2, heads // 2)
        return 2 * other + (side if k % 2 == 0 else 1 - side)

    shards = [shard_of(k) for k in range(heads)]
    distances = [jnp.abs(shard - me) for shard in shards]

    def rows(at, shard):
        return pl.ds(pl.multiple_of(at * block + shard * tokens, tokens), tokens)

    def part_of(k):
        return KEY if k == 1 else BOTH

    def own_copy(g, which):
        ref = (k_ref, v_ref)[which]
        return pltpu.make_async_copy(
            ref.at[:, pl.ds(pl.multiple_of(g * HEAD_SIZE, HEAD_SIZE), HEAD_SIZE)],
            kv.at[g, which, rows(2, me), :],
            own_sem.at[which, g],
        )

    def remote(g, part, source, landing, send, recv, place):
        return pltpu.make_async_remote_copy(
            src_ref=kv.at[g, part, source, :], dst_ref=kv.at[g, part, landing, :],
            send_sem=send, recv_sem=recv, device_id=place, device_id_type=MESH,
        )

    def z_own(g, k, part):
        at = rows(2, me)
        slot = (1 if k == 1 and part is VALUE else 0, k, g)
        recv = (1 if k == 1 and part is VALUE else 0, me, g)
        return remote(g, part, at, at, z_send.at[slot], z_recv.at[recv], {"head": shards[k]})

    def z_on(g, k):
        at = rows(2, shards[k])
        to = jnp.clip(me + jnp.where(shards[k] < me, 1, -1), 0, heads - 1)
        return remote(
            g, BOTH, at, at, on_send.at[k, g], z_recv.at[0, shards[k], g], {"head": to}
        )

    def z_goes_on(k):
        beyond = jnp.where(shards[k] < me, me + 1 < heads, me >= 1)
        return (distances[k] >= 2) & beyond

    def z_arrival(g, k, part):
        at = rows(2, shards[k])
        recv = (1 if k == 1 and part is VALUE else 0, shards[k], g)
        return remote(g, part, at, at, on_send.at[k, g], z_recv.at[recv], {"head": mate})

    def y_copy(g, k):
        return remote(
            g, part_of(k), rows(2, shards[k]), rows(0, shards[k]),
            y_send.at[k, g], y_recv.at[k, g], context(2),
        )

    def x_copy(g, k):
        return remote(
            g, part_of(k), rows(2 * (1 - odd), shards[k]), rows(1, shards[k]),
            x_send.at[k, g], x_recv.at[k, g], partner,
        )

    def pair_copy(g, at):
        return remote(
            g, VALUE, rows(at, me), rows(at, me), pair_send.at[at, g], pair_recv.at[at, g],
            {"head": mate},
        )

    def pair_arrival(g, at):
        return remote(
            g, VALUE, rows(at, mate), rows(at, mate), pair_send.at[at, g], pair_recv.at[at, g],
            {"head": mate},
        )

    def y_needed(k):
        return (odd == 1) | (shards[k] >= me)

    def have(g, k):
        @pl.when(y_needed(k))
        def _():
            y_copy(g, k).start()

        @pl.when(odd == 0)
        def _():
            x_copy(g, k).start()

    def x_own_event(g):
        @pl.when(odd == 0)
        def _():
            x_copy(g, 0).start()

    def y_own_event(g):
        y_copy(g, 0).start()

    def mate_event(g):
        z_own(g, 1, KEY).start()

    def mate_values_event(g):
        @pl.when(side == 0)
        def _():
            z_own(g, 1, VALUE).start()

    def pair_event(g):
        @pl.when(side == 1)
        def _():
            pair_copy(g, 0).start()

    def z_own_event(g, first):
        for k in range(first, heads, 2):
            @pl.when(distances[k] <= 2)
            def _():
                z_own(g, k, BOTH).start()

    def z_mate_event(g):
        z_arrival(g, 1, KEY).wait_recv()
        have(g, 1)

    def z_event(g, distance, which):
        for k in which:
            @pl.when(jnp.maximum(distances[k], 2) == distance)
            def _():
                z_arrival(g, k, BOTH).wait_recv()

                @pl.when(z_goes_on(k))
                def _():
                    z_on(g, k).start()

                have(g, k)

    def y_step(g, k):
        @pl.when(y_needed(k))
        def _():
            y_copy(g, k).wait_recv()

        @pl.when(odd == 1)
        def _():
            x_copy(g, k).start()

    def y_event(g, distance, which):
        for k in which:
            @pl.when(jnp.maximum(distances[k], 2) == distance)
            def _():
                y_step(g, k)

    def x_event(g):
        x_copy(g, 0).wait_recv()
        pair_copy(g, 1).start()

    def final_event(g):
        for k in range(1, heads):
            x_copy(g, k).wait_recv()
        pair_arrival(g, 1).wait_recv()

        @pl.when(side == 0)
        def _():
            pair_arrival(g, 0).wait_recv()

        @pl.when(side == 1)
        def _():
            z_arrival(g, 1, VALUE).wait_recv()

    def drain(g, carry):
        z_own(g, 1, KEY).wait_send()

        @pl.when(side == 0)
        def _():
            z_own(g, 1, VALUE).wait_send()

        for k in range(2, heads):
            @pl.when(distances[k] <= 2)
            def _():
                z_own(g, k, BOTH).wait_send()

            @pl.when(z_goes_on(k))
            def _():
                z_on(g, k).wait_send()

        for k in range(heads):
            @pl.when(y_needed(k))
            def _():
                y_copy(g, k).wait_send()

            x_copy(g, k).wait_send()

        pair_copy(g, 1).wait_send()

        @pl.when(side == 1)
        def _():
            pair_copy(g, 0).wait_send()

        return carry

    actions = {
        "x own": x_own_event, "y own": y_own_event, "z mate": mate_event,
        "z values": mate_values_event, "pair": pair_event,
        "z own": functools.partial(z_own_event, first=2),
        "z own odd": functools.partial(z_own_event, first=3),
        "z1": z_mate_event, "y0": functools.partial(y_step, k=0),
        "y1": functools.partial(y_step, k=1), "x0": x_event, "ready": final_event,
        "drain": lambda g: drain(g, 0),
    }
    even, uneven = range(2, heads, 2), range(3, heads, 2)
    for axis, event in (("z", z_event), ("y", y_event)):
        actions[axis + "2"] = functools.partial(event, distance=2, which=even)
        actions[axis + "2 odd"] = functools.partial(event, distance=2, which=uneven)
        for distance in range(3, heads):
            actions[axis + str(distance)] = functools.partial(
                event, distance=distance, which=range(2, heads)
            )

    slots = order_of(heads, groups, period)
    loads = list(dict.fromkeys(g for slot in slots for name, g in slot if name in OWN))

    q_copy = pltpu.make_async_copy(q_hbm, q_ref, q_sem)
    for g in loads:
        own_copy(g, 0).start()
        own_copy(g, 1).start()
    q_copy.start()

    barrier = pltpu.get_barrier_semaphore()
    for distance in range(1, heads):
        pl.semaphore_signal(
            barrier, inc=1, device_id={"head": lax.rem(me + distance, heads)}, device_id_type=MESH
        )
    for place in (context(2), context(-2), partner):
        pl.semaphore_signal(barrier, inc=1, device_id=place, device_id_type=MESH)
    pl.semaphore_wait(barrier, heads - 1 + 3)

    def documents(positions, lanes):
        number = jnp.zeros(positions.shape, jnp.int32)
        end = jnp.int32(0)
        for n in range(lengths_ref.shape[0]):
            end = end + lengths_ref[n]
            number = number + (positions >= end).astype(jnp.int32)
        return (number == lanes) & (positions >= 0)

    def fill_masks():
        first = ctx * block + me * tokens
        shape = (tokens, HEAD_SIZE)
        row = lax.broadcasted_iota(jnp.int32, shape, 0)
        lanes = lax.broadcasted_iota(jnp.int32, shape, 1)
        same = jnp.where(documents(first + row, lanes), 1.0, 0.0).astype(jnp.bfloat16)
        for p in range(pair):
            own_doc[p * tokens:(p + 1) * tokens, :] = same
        for n in range(2 * heads + 1):
            seen = documents(first - 2 * block + n * tokens + row, lanes)
            other_doc[n * tokens:(n + 1) * tokens, :] = jnp.where(seen, 0.0, -1e30).astype(jnp.bfloat16)
        shape = (tokens, tokens)
        later = lax.broadcasted_iota(jnp.int32, shape, 1) > lax.broadcasted_iota(jnp.int32, shape, 0)
        bias[...] = jnp.where(later, -1e30, 0.0)

    factor = math.log2(math.e) / math.sqrt(HEAD_SIZE)
    reading = pl.ds(pl.multiple_of(me * tokens, tokens), span)

    def columns_of(n):
        at = n * pair * HEAD_SIZE
        return [
            pl.ds(pl.multiple_of(at + p * HEAD_SIZE, HEAD_SIZE), HEAD_SIZE) for p in range(pair)
        ]

    def score(n, g, slot):
        q = jnp.concatenate([q_ref[:, c] for c in columns_of(n)], axis=0)
        q = jnp.concatenate([q, own_doc[...]], axis=1)
        key = jnp.concatenate([kv.at[g, 0][reading, :], other_doc[...]], axis=1)
        scores = lax.dot_general(
            q, key, (((1,), (1,)), ((), ())), preferred_element_type=jnp.float32
        )
        earlier = scores[:, :span - tokens]
        recent = scores[:, span - tokens:].reshape(pair, tokens, tokens) + bias[...][None]
        recent = recent.reshape(pair * tokens, tokens)
        held[slot][:, :span - tokens] = earlier
        held[slot][:, span - tokens:] = recent
        tops[slot][...] = jnp.maximum(
            jnp.max(earlier, axis=1, keepdims=True), jnp.max(recent, axis=1, keepdims=True)
        )

    def weigh(slot):
        weights = jnp.exp2((held[slot][...] - tops[slot][...]) * factor)
        totals[slot][...] = jnp.sum(weights, axis=1, keepdims=True)
        rounded[slot][...] = weights.astype(jnp.bfloat16)

    def attend(n, g, slot):
        summed = jnp.dot(
            rounded[slot][...], kv.at[g, 1][reading, :], preferred_element_type=jnp.float32
        )
        result = (summed / totals[slot][...]).astype(out_ref.dtype)
        for p, c in enumerate(columns_of(n)):
            out_ref[:, c] = result[p * tokens:(p + 1) * tokens]

    loaded = set()

    def take(slot):
        for name, g in slot:
            if g not in loaded:
                loaded.add(g)
                own_copy(g, 0).wait()
                own_copy(g, 1).wait()
            actions[name](g)

    def dispatch(step, low, high):
        if not any(slots[low:high]):
            return

        if high - low == 1:
            take(slots[low])
            return

        middle = (low + high) // 2

        @pl.when(step < middle)
        def _():
            dispatch(step, low, middle)

        @pl.when(step >= middle)
        def _():
            dispatch(step, middle, high)

    take(slots[0][:groups])
    fill_masks()
    take(slots[0][groups:])
    q_copy.wait()

    held[1][...] = jnp.zeros_like(held[1])
    tops[1][...] = jnp.zeros_like(tops[1])
    for slot in range(2):
        totals[slot][...] = jnp.ones_like(totals[slot])
        rounded[slot][...] = jnp.zeros_like(rounded[slot])

    def group_step(g, carry):
        def two_steps(i, carry):
            for slot in range(2):
                n = g * period + 2 * i + slot
                score(n, g, slot)
                weigh(1 - slot)
                attend(jnp.maximum(n - 2, 0), jnp.maximum(jnp.where(i > 0, g, g - 1), 0), slot)
                dispatch(n + 1, 1, steps + 1)
            return carry

        lax.fori_loop(0, period // 2, two_steps, 0)
        return carry

    lax.fori_loop(0, groups, group_step, 0)
    attend(steps - 2, groups - 1, 0)
    weigh(1)
    attend(steps - 1, groups - 1, 1)

    lax.fori_loop(max(groups - 2, 0), groups, drain, 0)


def solution(mesh):
    heads, outers, inners = (mesh.shape[name] for name in ("head", "outer", "inner"))

    def per_device(query, keys, values, lengths):
        tokens = query.shape[0]
        groups = keys.shape[1] // HEAD_SIZE
        sems = pltpu.SemaphoreType.DMA
        rows = pair_of(query.shape[1] // keys.shape[1]) * tokens
        return pl.pallas_call(
            functools.partial(kernel, heads, outers, inners),
            out_shape=pltpu.VMEM(query.shape, query.dtype),
            in_specs=[
                pl.BlockSpec(memory_space=pltpu.SMEM),
                pl.BlockSpec(memory_space=pl.ANY),
                pl.BlockSpec(memory_space=pl.ANY),
                pl.BlockSpec(memory_space=pl.ANY),
            ],
            out_specs=pl.BlockSpec(memory_space=pltpu.VMEM),
            scratch_shapes=[
                pltpu.VMEM(query.shape, query.dtype),
                pltpu.VMEM((groups, 2, 3 * heads * tokens, HEAD_SIZE), jnp.bfloat16),
                pltpu.VMEM((tokens, tokens), jnp.float32),
                pltpu.VMEM((rows, HEAD_SIZE), jnp.bfloat16),
                pltpu.VMEM(((2 * heads + 1) * tokens, HEAD_SIZE), jnp.bfloat16),
                [pltpu.VMEM((rows, (2 * heads + 1) * tokens), jnp.float32)] * 2,
                [pltpu.VMEM((rows, 1), jnp.float32)] * 2,
                [pltpu.VMEM((rows, 1), jnp.float32)] * 2,
                [pltpu.VMEM((rows, (2 * heads + 1) * tokens), jnp.bfloat16)] * 2,
                sems,
                sems((2, groups)),
                sems((2, heads, groups)),
                sems((2, heads, groups)),
                sems((heads, groups)),
                sems((heads, groups)),
                sems((heads, groups)),
                sems((heads, groups)),
                sems((heads, groups)),
                sems((2, groups)),
                sems((2, groups)),
            ],
            compiler_params=pltpu.CompilerParams(collective_id=0, has_side_effects=True),
        )(lengths, query, keys, values)

    rows = P(("outer", "inner", "head"), None)
    return jax.shard_map(
        per_device,
        mesh=mesh,
        in_specs=(rows, rows, rows, P()),
        out_specs=rows,
        check_vma=False,
    )
```
